32 devices in a mesh: outer: 4 (over y, x), inner: 8 (over z, core).
Axes of the slice: x: 2, y: 2, z: 4, core: 2. Of those that a mesh axis runs over, the one named last changes fastest.
Arguments:
- queries: bfloat16 [8192, 16, 128], P(('outer', 'inner')), may hold values from -6 to 6
- key_rows: bfloat16 [8192, 16, 128], P(('outer', 'inner')), may hold values from -6 to 6
- value_rows: bfloat16 [8192, 16, 128], P(('outer', 'inner')), may hold values from -6 to 6
- key_scale: bfloat16 [8192, 16], P(('outer', 'inner')), may hold values from 0.5 to 2
- value_scale: bfloat16 [8192, 16], P(('outer', 'inner')), may hold values from 0.5 to 2
- cluster_label: int32 [16, 8192, 1], P(None, ('outer', 'inner')), may hold values from 0 to 127; in each aligned block of 256 rows (0 to 255, 256 to 511, ..., all dimensions but the last counted through in order) at most 4 rows name the same one
Outputs:
- attended: bfloat16 [8192, 16, 128], P(('outer', 'inner'))
The draws below stay inside these ranges and needn't reach their ends.
Inputs may be any that keep to these rules, and one draw needn't show every extreme that they name: `cluster_label`: among the 256 rows of one device for one head, no label occurs more than 4 times, and some label occurs exactly 4 times.
All inputs are finite; a program needn't handle non-finite values.
Results may differ from the reference program's by a relative error of at most 0.0033.
Values may be sent and summed in bfloat16 or wider, within the bound.
A program may use at most 64 MiB of HBM per device.

```python
import math
import jax
import jax.numpy as jnp
import numpy as np
from jax import lax

HEADS = 16
HEAD = 128
COARSE = 16
FINE = 8
TOK_DEV = 256
CLUSTERS = 128
CAP = 4
TOKENS = 8192
N_OUTER = 4
N_INNER = 8


def draw_vectors(key, fold_tag):
    drawn = jax.random.normal(jax.random.fold_in(key, fold_tag), (TOKENS, HEADS, HEAD), jnp.float32)
    return jnp.clip(drawn, -6.0, 6.0).astype(jnp.bfloat16)


def draw_queries(key, part):
    return draw_vectors(key, 11)


def draw_key_rows(key, part):
    return draw_vectors(key, 13)


def levels(own_key, dims, pieces, low, high):
    gain = 1.0
    for axis_at, blocks in pieces:
        steps = jax.random.uniform(jax.random.fold_in(jax.random.fold_in(own_key, 6), axis_at), (blocks,), jnp.float32, low / len(pieces), high / len(pieces))
        gain = gain * jnp.repeat(jnp.exp(steps), dims[axis_at] // blocks).reshape((-1,) + (1,) * (len(dims) - 1 - axis_at))
    return gain


def routed_block(rng, own, number, rows, amount, top, reach, lean):
    sequence = jax.random.permutation(rng, amount)
    heavy_load, ordinary = shares(amount, rows * top, reach, lean, True), shares(amount, rows * top, reach, lean, False)
    places = jnp.arange(amount)

    def named(sizes, offset_by):
        used = int((sizes > 0).sum())
        fixed = max(1, used // 4)
        shifted = fixed + (places - fixed + offset_by * (used - fixed)) % max(1, amount - fixed)
        return jnp.zeros((amount,), jnp.int32).at[sequence[jnp.where(places < fixed, places, shifted)]].set(jnp.asarray(sizes, jnp.int32))

    sizes = jnp.where(number % 4 == 0, named(heavy_load, number // 4), named(ordinary, number - number // 4 - 1))
    mixed = jax.random.permutation(jax.random.fold_in(own, 3), amount)
    donor, receiver = mixed[0:amount // 2 * 2:2], mixed[1:amount // 2 * 2:2]
    margin = jnp.minimum(sizes[donor] - 1, reach - sizes[receiver]) // 2
    margin = jnp.where((donor == sequence[0]) | (receiver == sequence[0]) | (sizes[receiver] == 0), 0, jnp.maximum(margin, 0))
    shifted = jax.random.randint(jax.random.fold_in(own, 4), (amount // 2,), 0, 1 << 20) % (margin + 1)
    sizes = sizes.at[donor].add(-shifted).at[receiver].add(shifted)
    items = jnp.searchsorted(jnp.cumsum(sizes), jnp.arange(rows * top), side="right").astype(jnp.int32)
    table = items.reshape(top, rows).T
    table = table[jax.random.permutation(jax.random.fold_in(own, 1), rows)]
    offset_by = jax.random.randint(jax.random.fold_in(own, 2), (rows, 1), 0, top)
    return jnp.take_along_axis(table, (jnp.arange(top)[None, :] + offset_by) % top, axis=1)


def shares(count, total, most, slope, full):
    loads = [(1 << 20) // math.isqrt(rank ** slope) + 1 for rank in range(1, count + 1)]
    largest = most if full else min(most, max(-(-total // count), total * loads[0] // sum(loads)))
    least = 1 if total - largest >= count - 1 else 0
    holding, spare = [largest] + [least] * (count - 1), total - largest - least * (count - 1)
    while spare > 0:
        free = [i for i in range(1, count) if holding[i] < largest] or [i for i in range(1, count) if holding[i] < most]
        mass, budget = sum([loads[i] for i in free]), spare
        for i in free:
            addition = min(most - holding[i], max(1, budget * loads[i] // mass), spare)
            holding[i] = holding[i] + addition
            spare = spare - addition
    return np.array(holding)


def noise(rng, dims, scale, reach, split=(), kind=jnp.bfloat16):
    loudness = levels(rng, dims, split, -0.22, 0.18) if split else 1.0
    values = jax.random.normal(rng, dims, jnp.float32) * scale * loudness
    return jnp.minimum(jnp.maximum(values, -reach), reach).astype(kind)


def setup_inputs(seed: int = 0) -> dict:
    arg_keys = jax.random.split(jax.random.key(seed), 7)
    queries = draw_queries(jax.random.fold_in(arg_keys[6], 71), 0)
    key_rows = draw_key_rows(jax.random.fold_in(arg_keys[6], 71), 0)
    value_rows = noise(arg_keys[2], (TOKENS, HEADS, HEAD), 1.0, 6.0, ((0, 32),))
    key_scale = jnp.clip(jnp.exp(math.log(2.0) - 1.3862944 * jax.random.uniform(arg_keys[3], (TOKENS, HEADS), jnp.float32) ** levels(arg_keys[3], (TOKENS, HEADS), ((0, 32),), -0.2, 0.2)), 0.5, 2.0).astype(jnp.bfloat16)
    value_scale = jnp.clip(jnp.exp(math.log(2.0) - 1.3862944 * jax.random.uniform(arg_keys[4], (TOKENS, HEADS), jnp.float32) ** levels(arg_keys[4], (TOKENS, HEADS), ((0, 32),), -0.2, 0.2)), 0.5, 2.0).astype(jnp.bfloat16)
    cluster_label_keys = jax.random.split(jax.random.fold_in(arg_keys[5], 1), HEADS * TOKENS // TOK_DEV)
    cluster_label_turns = jax.random.permutation(jax.random.fold_in(arg_keys[5], 3), HEADS * TOKENS // TOK_DEV)
    cluster_label = jax.vmap(lambda own, number: routed_block(jax.random.fold_in(arg_keys[5], 2), own, number, TOK_DEV, CLUSTERS, 1, CAP, 2))(cluster_label_keys, cluster_label_turns).reshape((HEADS, TOKENS, 1))
    return dict(queries=queries, key_rows=key_rows, value_rows=value_rows, key_scale=key_scale, value_scale=value_scale, cluster_label=cluster_label)


def attend(query_block, key_block, value_block, key_factor, value_factor, position):
    factor = query_block.shape[-1] ** -0.5
    scores = jnp.dot(query_block, key_block.T, preferred_element_type=jnp.float32)
    scores = scores * (key_factor.astype(jnp.float32) * factor)[None, :]
    visible = (position[None, :] >= 0) & (position[None, :] <= position[:, None])
    highest = jnp.max(jnp.where(visible, scores, jnp.float32(-1e30)), axis=1, keepdims=True)
    unnormed = jnp.where(visible, jnp.exp(scores - highest), jnp.float32(0.0))
    denominator = jnp.sum(unnormed, axis=1)
    weights = (unnormed * value_factor.astype(jnp.float32)[None, :]).astype(jnp.bfloat16)
    numerator = jnp.dot(weights, value_block, preferred_element_type=jnp.float32)
    safe = jnp.where(denominator > 0, denominator, jnp.float32(1.0))
    return (numerator / safe[:, None]).astype(jnp.bfloat16)


def reference(queries, key_rows, value_rows, key_scale, value_scale, cluster_label):
    cluster_count = COARSE * FINE
    window = N_OUTER * N_INNER * CAP
    token_count = queries.shape[0]
    width = queries.shape[2]

    def per_head(inputs):
        query_head, key_head, value_head, key_factor, value_factor, labels = inputs
        order = jnp.argsort(labels, stable=True).astype(jnp.int32)
        counts = jnp.zeros((cluster_count,), jnp.int32).at[labels].add(1)
        starts = jnp.cumsum(counts) - counts

        def per_cluster(which):
            offset = jnp.arange(window, dtype=jnp.int32)
            inside = offset < counts[which]
            token = order[jnp.minimum(starts[which] + offset, token_count - 1)]
            position = jnp.where(inside, token, -1).astype(jnp.int32)
            result = attend(query_head[token], key_head[token], value_head[token],
                            key_factor[token], value_factor[token], position)
            target = jnp.where(inside, token, token_count).astype(jnp.int32)
            return result, target

        results, targets = lax.map(per_cluster, jnp.arange(cluster_count, dtype=jnp.int32))
        empty = jnp.zeros((token_count, width), jnp.bfloat16)
        return empty.at[targets.reshape(-1)].set(results.reshape(-1, width), mode="drop")

    stacked = lax.map(per_head, (jnp.swapaxes(queries, 0, 1), jnp.swapaxes(key_rows, 0, 1),
                                 jnp.swapaxes(value_rows, 0, 1), key_scale.T, value_scale.T,
                                 cluster_label[:, :, 0]))
    return jnp.swapaxes(stacked, 0, 1)
```

```python
import jax
import jax.numpy as jnp
from jax import lax
from jax.experimental import pallas as pl
from jax.experimental.pallas import tpu as pltpu
from jax.sharding import PartitionSpec as P

COARSE = 16
FINE = 8


def attend(query_block, key_block, value_block, key_factor, value_factor, position):
    factor = query_block.shape[-1] ** (-0.5)
    scores = jnp.dot(query_block, key_block.T, preferred_element_type=jnp.float32)
    scores = scores * (key_factor.astype(jnp.float32) * factor)[None, :]
    visible = (position[None, :] >= 0) & (position[None, :] <= position[:, None])
    highest = jnp.max(jnp.where(visible, scores, jnp.float32(-1e30)), axis=1, keepdims=True)
    unnormed = jnp.where(visible, jnp.exp(scores - highest), jnp.float32(0.0))
    denominator = jnp.sum(unnormed, axis=1)
    weights = (unnormed * value_factor.astype(jnp.float32)[None, :]).astype(jnp.bfloat16)
    numerator = jnp.dot(weights, value_block, preferred_element_type=jnp.float32)
    safe = jnp.where(denominator > 0, denominator, jnp.float32(1.0))
    return (numerator / safe[:, None]).astype(jnp.bfloat16)


def attend_items(query_part, key_part, value_part, key_factor, value_factor, position):
    leading = query_part.shape[:3]
    slots = query_part.shape[3]
    width = query_part.shape[4]
    total = leading[0] * leading[1] * leading[2]

    def single(inputs):
        return attend(*inputs)

    results = lax.map(
        single,
        (
            query_part.reshape(total, slots, width),
            key_part.reshape(total, slots, width),
            value_part.reshape(total, slots, width),
            key_factor.reshape(total, slots),
            value_factor.reshape(total, slots),
            position.reshape(total, slots),
        ),
    )
    return results.reshape(leading + (slots, width))


def shards(queries, key_rows, value_rows, key_scale, value_scale, cluster_label):
    outer_count = lax.axis_size("outer")
    inner_count = lax.axis_size("inner")
    tok_rows, heads, width = queries.shape
    cluster_count = COARSE * FINE
    capacity = max(2, 2 * tok_rows // cluster_count)
    labels = cluster_label[:, :, 0].T
    member = (
        labels[:, :, None] == jnp.arange(cluster_count, dtype=jnp.int32)[None, None, :]
    ).astype(jnp.int32)
    rank = jnp.sum(jnp.cumsum(member, axis=0) * member, axis=2) - 1
    slot = (labels * heads + jnp.arange(heads, dtype=jnp.int32)[None, :]) * capacity + rank
    flat = slot.reshape(-1)
    total = cluster_count * heads * capacity
    item_count = cluster_count * heads // (outer_count * inner_count)
    layout = (outer_count, inner_count, item_count, capacity)
    source = (
        jnp.full((total,), -1, jnp.int32)
        .at[flat]
        .set(jnp.arange(tok_rows * heads, dtype=jnp.int32))
    )
    filled_slot = source >= 0
    source_row = jnp.maximum(source, 0)

    def place(array):
        rows = array.reshape((tok_rows * heads,) + array.shape[2:])
        picked = rows[source_row]
        mask = filled_slot.reshape((total,) + (1,) * (picked.ndim - 1))
        kept = jnp.where(mask, picked, jnp.zeros((), array.dtype))
        return kept.reshape(layout + array.shape[2:])

    device = lax.axis_index("outer") * inner_count + lax.axis_index("inner")
    position_rows = jnp.where(filled_slot, device * tok_rows + source_row // heads, -1).reshape(
        layout
    )
    outgoing = (
        place(queries),
        place(key_rows),
        place(value_rows),
        place(key_scale),
        place(value_scale),
        position_rows,
    )
    arrived = (
        lax.all_to_all(
            lax.all_to_all(outgoing[0], "outer", split_axis=0, concat_axis=3, tiled=True),
            "inner",
            split_axis=1,
            concat_axis=3,
            tiled=True,
        ),
        lax.all_to_all(
            lax.all_to_all(outgoing[1], "outer", split_axis=0, concat_axis=3, tiled=True),
            "inner",
            split_axis=1,
            concat_axis=3,
            tiled=True,
        ),
        lax.all_to_all(
            lax.all_to_all(outgoing[2], "outer", split_axis=0, concat_axis=3, tiled=True),
            "inner",
            split_axis=1,
            concat_axis=3,
            tiled=True,
        ),
        lax.all_to_all(
            lax.all_to_all(outgoing[3], "outer", split_axis=0, concat_axis=3, tiled=True),
            "inner",
            split_axis=1,
            concat_axis=3,
            tiled=True,
        ),
        lax.all_to_all(
            lax.all_to_all(outgoing[4], "outer", split_axis=0, concat_axis=3, tiled=True),
            "inner",
            split_axis=1,
            concat_axis=3,
            tiled=True,
        ),
        lax.all_to_all(
            lax.all_to_all(outgoing[5], "outer", split_axis=0, concat_axis=3, tiled=True),
            "inner",
            split_axis=1,
            concat_axis=3,
            tiled=True,
        ),
    )
    answered = attend_items(*arrived)
    returned = lax.all_to_all(
        lax.all_to_all(answered, "inner", split_axis=3, concat_axis=1, tiled=True),
        "outer",
        split_axis=3,
        concat_axis=0,
        tiled=True,
    )
    rows_back = returned.reshape(total, width)
    return rows_back[flat].reshape(tok_rows, heads, width)

AUX = 16


def exchange_kernel(
    chips, half, tok, slots, x_ref, o_ref, recv, ans, kp, vp, xp, qp, op, vis_ref,
    send_sem, recv_sem, fsend, frecv, bsend, brecv,
):
    f32, bf16 = jnp.float32, jnp.bfloat16
    width = x_ref.shape[2]
    inner = lax.axis_index("inner")
    chip = lax.axis_index("outer") * half + inner // 2
    core = inner % 2
    partner = {"outer": lax.axis_index("outer"), "inner": inner + 1 - 2 * core}
    head_rows = pl.ds(tok, x_ref.shape[1] - tok)

    def at(other):
        return {"outer": other // half, "inner": (other % half) * 2 + core}

    def copy(src, dst, s1, s2, where):
        return pltpu.make_async_remote_copy(
            src_ref=src, dst_ref=dst, send_sem=s1, recv_sem=s2,
            device_id=where, device_id_type=pl.DeviceIdType.MESH,
        )

    barrier = pltpu.get_barrier_semaphore()

    @pl.loop(1, chips)
    def _(d):
        pl.semaphore_signal(
            barrier, inc=1, device_id=at((chip + d) % chips),
            device_id_type=pl.DeviceIdType.MESH,
        )

    pl.semaphore_signal(
        barrier, inc=1, device_id=partner, device_id_type=pl.DeviceIdType.MESH
    )
    pl.semaphore_wait(barrier, chips)

    def outgoing(d):
        other = (chip + d) % chips
        return copy(
            x_ref.at[other], recv.at[2 * chip + core], send_sem.at[d], recv_sem.at[d], at(other)
        )

    @pl.loop(1, chips)
    def _(d):
        outgoing(d).start()

    def source(d):
        return (chip + chips - d) % chips

    def own_forward():
        return copy(
            x_ref.at[chip, head_rows], recv.at[2 * chip + core, head_rows],
            fsend.at[0], frecv.at[0], partner,
        )

    def forward(d):
        row = 2 * source(d) + core
        return copy(
            recv.at[row, head_rows], recv.at[row, head_rows], fsend.at[d], frecv.at[d], partner
        )

    own_forward().start()
    recv[2 * chip + core] = x_ref[chip]

    lane = lax.broadcasted_iota(jnp.int32, (tok, width), 1)
    low = (lane < width // 2).astype(f32).astype(bf16)
    high = (lane >= width // 2).astype(f32).astype(bf16)
    key_at = lax.broadcasted_iota(jnp.int32, vis_ref.shape, 1)
    query_at = lax.broadcasted_iota(jnp.int32, vis_ref.shape, 0)
    key_order = (key_at // 8) * 4 + key_at % 4
    query_order = (2 * (query_at // 8) + core) * 4 + query_at % 4
    same = (key_at // 4) % 2 == (query_at // 4) % 2
    vis_ref[...] = jnp.where(same & (key_order <= query_order), f32(1.0), f32(0.0))
    halves = tok // width

    def aux_of(row):
        return jnp.concatenate(
            [recv[row, pl.ds(3 * tok + AUX * i, AUX)] for i in range(halves)], axis=1
        )

    def place(row, with_query):
        aux = aux_of(row).astype(f32)
        slot = (aux[2:3] + aux[3:4]).astype(jnp.int32)
        hit = lax.broadcasted_iota(jnp.int32, (slots, tok), 0) == slot
        one = jnp.where(hit, f32(1.0), f32(0.0)).astype(bf16)
        by_key = jnp.where(hit, aux[0:1], f32(0.0)).astype(bf16)
        by_value = jnp.where(hit, aux[1:2], f32(0.0)).astype(bf16)
        kp[row] = jnp.dot(one, recv[row, pl.ds(tok, tok)], preferred_element_type=f32)
        vp[row] = jnp.dot(one, recv[row, pl.ds(2 * tok, tok)], preferred_element_type=f32)
        xp[row] = jnp.dot(by_key, low, preferred_element_type=f32) + jnp.dot(
            by_value, high, preferred_element_type=f32
        )
        if with_query:
            qp[row // 2] = jnp.dot(one, recv[row, pl.ds(0, tok)], preferred_element_type=f32)

    place(2 * chip + core, True)

    @pl.loop(1, chips)
    def _(d):
        outgoing(d).wait_recv()
        forward(d).start()
        place(2 * source(d) + core, True)

        @pl.when(d == 1)
        def _():
            own_forward().wait_recv()

        @pl.when(d > 1)
        def _():
            forward(d - 1).wait_recv()

        place(2 * source(d - 1) + 1 - core, False)

    forward(chips - 1).wait_recv()
    place(2 * source(chips - 1) + 1 - core, False)

    sel_lane = lax.broadcasted_iota(jnp.int32, (16, width), 1)
    sel_row = lax.broadcasted_iota(jnp.int32, (16, width), 0)
    select = (sel_lane == jnp.where(sel_row < 8, 0, width // 2)).astype(f32).astype(bf16)
    factor = width ** (-0.5)
    queries_here, keys_here = vis_ref.shape

    def group(t):
        rows = pl.ds(pl.multiple_of(t * 8, 8), 8)
        key = kp[:, rows, :].reshape(keys_here, width).astype(bf16)
        value = vp[:, rows, :].reshape(keys_here, width).astype(bf16)
        extra = xp[:, rows, :].reshape(keys_here, width).astype(bf16)
        query = qp[:, rows, :].reshape(queries_here, width).astype(bf16)
        nt = (((1,), (1,)), ((), ()))
        scale = lax.dot_general(select, extra, nt, preferred_element_type=f32)
        scores = lax.dot_general(query, key, nt, preferred_element_type=f32)
        scores = scores * (scale[0:1] * factor)
        visible = vis_ref[...] * scale[0:1] > 0
        scores = jnp.where(visible, scores, f32(-1e30))
        highest = jnp.max(scores, axis=1, keepdims=True)
        unnormed = jnp.where(visible, jnp.exp(scores - highest), f32(0.0))
        denominator = jnp.sum(unnormed, axis=1, keepdims=True)
        weights = (unnormed * scale[8:9]).astype(bf16)
        numerator = jnp.dot(weights, value, preferred_element_type=f32)
        safe = jnp.where(denominator > 0, denominator, f32(1.0))
        result = (numerator / safe).astype(bf16).astype(f32)
        op[:, rows, :] = result.reshape(queries_here // 8, 8, width)

    @pl.loop(0, slots // 8 // UNROLL)
    def _(t):
        for u in range(UNROLL):
            group(t * UNROLL + u)

    eye = (
        lax.broadcasted_iota(jnp.int32, (tok, tok), 0)
        == lax.broadcasted_iota(jnp.int32, (tok, tok), 1)
    ).astype(f32).astype(bf16)

    def answer(other):
        columns = lax.dot_general(
            eye, aux_of(2 * other + core), (((1,), (1,)), ((), ())), preferred_element_type=f32
        )
        slot = (columns[:, 2:3] + columns[:, 3:4]).astype(jnp.int32)
        hit = lax.broadcasted_iota(jnp.int32, (tok, slots), 1) == slot
        one = jnp.where(hit, f32(1.0), f32(0.0)).astype(bf16)
        return jnp.dot(one, op[other].astype(bf16), preferred_element_type=f32).astype(bf16)

    def reply(d):
        other = (chip + d) % chips
        return copy(ans.at[other], o_ref.at[chip], bsend.at[d], brecv.at[d], at(other))

    @pl.loop(1, chips)
    def _(d):
        other = (chip + d) % chips
        ans[other] = answer(other)

        @pl.when(d > 1)
        def _():
            reply(d - 1).start()

    o_ref[chip] = answer(chip)
    reply(chips - 1).start()
    own_forward().wait_send()

    @pl.loop(1, chips)
    def _(d):
        outgoing(d).wait_send()
        forward(d).wait_send()
        reply(d).wait()


def by_head(queries, key_rows, value_rows, key_scale, value_scale, cluster_label):
    tok, heads, width = queries.shape
    half = lax.axis_size("inner") // 2
    chips = lax.axis_size("outer") * half
    clusters = COARSE * FINE
    capacity = max(2, 2 * tok // clusters)
    slots = clusters * capacity
    labels = cluster_label[:, :, 0]
    earlier = jnp.arange(tok)[None, :] < jnp.arange(tok)[:, None]
    rank = jnp.sum(
        ((labels[:, :, None] == labels[:, None, :]) & earlier[None]).astype(jnp.int32), axis=2
    )
    aux = jnp.stack(
        [
            key_scale.T,
            value_scale.T,
            (labels * capacity).astype(jnp.bfloat16),
            rank.astype(jnp.bfloat16),
        ],
        axis=1,
    )
    aux = jnp.pad(aux, ((0, 0), (0, AUX - 4), (0, 0)))
    aux = aux.reshape(heads, AUX, tok // width, width).swapaxes(1, 2).reshape(heads, -1, width)
    packed = jnp.concatenate(
        [
            queries.swapaxes(0, 1),
            key_rows.swapaxes(0, 1),
            value_rows.swapaxes(0, 1),
            aux,
        ],
        axis=1,
    )
    vm = pl.BlockSpec(memory_space=pltpu.VMEM)
    dma = pltpu.SemaphoreType.DMA
    f32 = jnp.float32
    returned = pl.pallas_call(
        lambda *refs: exchange_kernel(chips, half, tok, slots, *refs),
        out_shape=jax.ShapeDtypeStruct((heads, tok, width), jnp.bfloat16),
        in_specs=[vm],
        out_specs=vm,
        scratch_shapes=[
            pltpu.VMEM((2 * chips,) + packed.shape[1:], jnp.bfloat16),
            pltpu.VMEM((chips, tok, width), jnp.bfloat16),
            pltpu.VMEM((2 * chips, slots, width), f32),
            pltpu.VMEM((2 * chips, slots, width), f32),
            pltpu.VMEM((2 * chips, slots, width), f32),
            pltpu.VMEM((chips, slots, width), f32),
            pltpu.VMEM((chips, slots, width), f32),
            pltpu.VMEM((8 * chips, 16 * chips), f32),
        ]
        + [dma((chips,))] * 6,
        compiler_params=pltpu.CompilerParams(
            collective_id=0, has_side_effects=True, vmem_limit_bytes=62 * 1024 * 1024
        ),
        name="clustered",
    )(packed)
    return returned.swapaxes(0, 1)


UNROLL = 2


def route(queries, key_rows, value_rows, key_scale, value_scale, cluster_label):
    tok, heads, width = queries.shape
    devices = lax.axis_size("outer") * lax.axis_size("inner")
    even = lax.axis_size("inner") % 2 == 0 and tok % width == 0
    if devices == 2 * heads and even and 2 * tok == 4 * COARSE * FINE:
        return by_head(queries, key_rows, value_rows, key_scale, value_scale, cluster_label)
    return shards(queries, key_rows, value_rows, key_scale, value_scale, cluster_label)


def solution(mesh):
    placed = (
        P(("outer", "inner"), None, None),
        P(("outer", "inner"), None, None),
        P(("outer", "inner"), None, None),
        P(("outer", "inner"), None),
        P(("outer", "inner"), None),
        P(None, ("outer", "inner"), None),
    )
    return jax.shard_map(
        route,
        mesh=mesh,
        in_specs=placed,
        out_specs=P(("outer", "inner"), None, None),
        check_vma=False,
    )
```

```python
import jax
import jax.numpy as jnp
from jax import lax
from jax.experimental import pallas as pl
from jax.experimental.pallas import tpu as pltpu
from jax.sharding import PartitionSpec as P

COARSE = 16
FINE = 8


def attend(query_block, key_block, value_block, key_factor, value_factor, position):
    factor = query_block.shape[-1] ** (-0.5)
    scores = jnp.dot(query_block, key_block.T, preferred_element_type=jnp.float32)
    scores = scores * (key_factor.astype(jnp.float32) * factor)[None, :]
    visible = (position[None, :] >= 0) & (position[None, :] <= position[:, None])
    highest = jnp.max(jnp.where(visible, scores, jnp.float32(-1e30)), axis=1, keepdims=True)
    unnormed = jnp.where(visible, jnp.exp(scores - highest), jnp.float32(0.0))
    denominator = jnp.sum(unnormed, axis=1)
    weights = (unnormed * value_factor.astype(jnp.float32)[None, :]).astype(jnp.bfloat16)
    numerator = jnp.dot(weights, value_block, preferred_element_type=jnp.float32)
    safe = jnp.where(denominator > 0, denominator, jnp.float32(1.0))
    return (numerator / safe[:, None]).astype(jnp.bfloat16)


def attend_items(query_part, key_part, value_part, key_factor, value_factor, position):
    leading = query_part.shape[:3]
    slots = query_part.shape[3]
    width = query_part.shape[4]
    total = leading[0] * leading[1] * leading[2]

    def single(inputs):
        return attend(*inputs)

    results = lax.map(
        single,
        (
            query_part.reshape(total, slots, width),
            key_part.reshape(total, slots, width),
            value_part.reshape(total, slots, width),
            key_factor.reshape(total, slots),
            value_factor.reshape(total, slots),
            position.reshape(total, slots),
        ),
    )
    return results.reshape(leading + (slots, width))


def shards(queries, key_rows, value_rows, key_scale, value_scale, cluster_label):
    outer_count = lax.axis_size("outer")
    inner_count = lax.axis_size("inner")
    tok_rows, heads, width = queries.shape
    cluster_count = COARSE * FINE
    capacity = max(2, 2 * tok_rows // cluster_count)
    labels = cluster_label[:, :, 0].T
    member = (
        labels[:, :, None] == jnp.arange(cluster_count, dtype=jnp.int32)[None, None, :]
    ).astype(jnp.int32)
    rank = jnp.sum(jnp.cumsum(member, axis=0) * member, axis=2) - 1
    slot = (labels * heads + jnp.arange(heads, dtype=jnp.int32)[None, :]) * capacity + rank
    flat = slot.reshape(-1)
    total = cluster_count * heads * capacity
    item_count = cluster_count * heads // (outer_count * inner_count)
    layout = (outer_count, inner_count, item_count, capacity)
    source = (
        jnp.full((total,), -1, jnp.int32)
        .at[flat]
        .set(jnp.arange(tok_rows * heads, dtype=jnp.int32))
    )
    filled_slot = source >= 0
    source_row = jnp.maximum(source, 0)

    def place(array):
        rows = array.reshape((tok_rows * heads,) + array.shape[2:])
        picked = rows[source_row]
        mask = filled_slot.reshape((total,) + (1,) * (picked.ndim - 1))
        kept = jnp.where(mask, picked, jnp.zeros((), array.dtype))
        return kept.reshape(layout + array.shape[2:])

    device = lax.axis_index("outer") * inner_count + lax.axis_index("inner")
    position_rows = jnp.where(filled_slot, device * tok_rows + source_row // heads, -1).reshape(
        layout
    )
    outgoing = (
        place(queries),
        place(key_rows),
        place(value_rows),
        place(key_scale),
        place(value_scale),
        position_rows,
    )
    arrived = (
        lax.all_to_all(
            lax.all_to_all(outgoing[0], "outer", split_axis=0, concat_axis=3, tiled=True),
            "inner",
            split_axis=1,
            concat_axis=3,
            tiled=True,
        ),
        lax.all_to_all(
            lax.all_to_all(outgoing[1], "outer", split_axis=0, concat_axis=3, tiled=True),
            "inner",
            split_axis=1,
            concat_axis=3,
            tiled=True,
        ),
        lax.all_to_all(
            lax.all_to_all(outgoing[2], "outer", split_axis=0, concat_axis=3, tiled=True),
            "inner",
            split_axis=1,
            concat_axis=3,
            tiled=True,
        ),
        lax.all_to_all(
            lax.all_to_all(outgoing[3], "outer", split_axis=0, concat_axis=3, tiled=True),
            "inner",
            split_axis=1,
            concat_axis=3,
            tiled=True,
        ),
        lax.all_to_all(
            lax.all_to_all(outgoing[4], "outer", split_axis=0, concat_axis=3, tiled=True),
            "inner",
            split_axis=1,
            concat_axis=3,
            tiled=True,
        ),
        lax.all_to_all(
            lax.all_to_all(outgoing[5], "outer", split_axis=0, concat_axis=3, tiled=True),
            "inner",
            split_axis=1,
            concat_axis=3,
            tiled=True,
        ),
    )
    answered = attend_items(*arrived)
    returned = lax.all_to_all(
        lax.all_to_all(answered, "inner", split_axis=3, concat_axis=1, tiled=True),
        "outer",
        split_axis=3,
        concat_axis=0,
        tiled=True,
    )
    rows_back = returned.reshape(total, width)
    return rows_back[flat].reshape(tok_rows, heads, width)

AUX = 8


def exchange_kernel(
    chips, half, tok, slots, x_ref, o_ref, recv, ans, kp, vp, xp, qp, op, held, vis_ref,
    send_sem, recv_sem, fsend, frecv, vsend, vrecv, vfsend, vfrecv, bsend, brecv,
):
    f32, bf16 = jnp.float32, jnp.bfloat16
    width = x_ref.shape[2]
    inner = lax.axis_index("inner")
    chip = lax.axis_index("outer") * half + inner // 2
    core = inner % 2
    partner = {"outer": lax.axis_index("outer"), "inner": inner + 1 - 2 * core}
    first = x_ref.shape[1] - tok
    first_rows, key_rows, value_rows = pl.ds(0, first), pl.ds(tok, first - tok), pl.ds(first, tok)

    def at(other):
        return {"outer": other // half, "inner": (other % half) * 2 + core}

    def copy(src, dst, s1, s2, where):
        return pltpu.make_async_remote_copy(
            src_ref=src, dst_ref=dst, send_sem=s1, recv_sem=s2,
            device_id=where, device_id_type=pl.DeviceIdType.MESH,
        )

    barrier = pltpu.get_barrier_semaphore()

    @pl.loop(1, chips)
    def _(d):
        pl.semaphore_signal(
            barrier, inc=1, device_id=at((chip + d) % chips),
            device_id_type=pl.DeviceIdType.MESH,
        )

    pl.semaphore_signal(
        barrier, inc=1, device_id=partner, device_id_type=pl.DeviceIdType.MESH
    )
    pl.semaphore_wait(barrier, chips)

    def outgoing(d):
        other = (chip + d) % chips
        return copy(
            x_ref.at[other, first_rows], recv.at[2 * chip + core, first_rows],
            send_sem.at[d], recv_sem.at[d], at(other),
        )

    def outgoing_value(d):
        other = (chip + d) % chips
        return copy(
            x_ref.at[other, value_rows], recv.at[2 * chip + core, value_rows],
            vsend.at[d], vrecv.at[d], at(other),
        )

    @pl.loop(1, chips)
    def _(d):
        outgoing(d).start()

    @pl.loop(1, chips)
    def _(d):
        outgoing_value(d).start()

    def source(d):
        return (chip + chips - d) % chips

    def own_forward(rows, s1, s2):
        return copy(
            x_ref.at[chip, rows], recv.at[2 * chip + core, rows], s1.at[0], s2.at[0], partner
        )

    def forward(d, rows, s1, s2):
        row = 2 * source(d) + core
        return copy(recv.at[row, rows], recv.at[row, rows], s1.at[d], s2.at[d], partner)

    by_keys, by_values = (key_rows, fsend, frecv), (value_rows, vfsend, vfrecv)
    own_forward(*by_keys).start()
    own_forward(*by_values).start()
    recv[2 * chip + core] = x_ref[chip]

    lane = lax.broadcasted_iota(jnp.int32, (tok, width), 1)
    low = (lane < width // 2).astype(f32).astype(bf16)
    high = (lane >= width // 2).astype(f32).astype(bf16)
    key_at = lax.broadcasted_iota(jnp.int32, vis_ref.shape, 1)
    query_at = lax.broadcasted_iota(jnp.int32, vis_ref.shape, 0)
    key_order = (key_at // 8) * 4 + key_at % 4
    query_order = (2 * (query_at // 8) + core) * 4 + query_at % 4
    same = (key_at // 4) % 2 == (query_at // 4) % 2
    vis_ref[...] = jnp.where(same & (key_order <= query_order), f32(1.0), f32(0.0))
    halves = tok // width

    def aux_of(row):
        block = recv[row, pl.ds(2 * tok, AUX * halves)].astype(f32)
        return jnp.concatenate(
            [block[AUX * i : AUX * (i + 1)] for i in range(halves)], axis=1
        )

    def hits(aux):
        slot = (aux[2:3] + aux[3:4]).astype(jnp.int32)
        return lax.broadcasted_iota(jnp.int32, (slots, tok), 0) == slot

    def place(row, with_query):
        aux = aux_of(row)
        hit = hits(aux)
        one = jnp.where(hit, f32(1.0), f32(0.0)).astype(bf16)
        by_key = jnp.where(hit, aux[0:1], f32(0.0)).astype(bf16)
        by_value = jnp.where(hit, aux[1:2], f32(0.0)).astype(bf16)
        kp[row] = jnp.dot(one, recv[row, pl.ds(tok, tok)], preferred_element_type=f32)
        xp[row] = jnp.dot(by_key, low, preferred_element_type=f32) + jnp.dot(
            by_value, high, preferred_element_type=f32
        )
        if with_query:
            qp[row // 2] = jnp.dot(one, recv[row, pl.ds(0, tok)], preferred_element_type=f32)

    def place_value(row):
        one = jnp.where(hits(aux_of(row)), f32(1.0), f32(0.0)).astype(bf16)
        vp[row] = jnp.dot(one, recv[row, value_rows], preferred_element_type=f32)

    place(2 * chip + core, True)

    @pl.loop(1, chips)
    def _(d):
        outgoing(d).wait_recv()
        forward(d, *by_keys).start()
        place(2 * source(d) + core, True)

        @pl.when(d == 1)
        def _():
            own_forward(*by_keys).wait_recv()

        @pl.when(d > 1)
        def _():
            forward(d - 1, *by_keys).wait_recv()

        place(2 * source(d - 1) + 1 - core, False)

    forward(chips - 1, *by_keys).wait_recv()
    place(2 * source(chips - 1) + 1 - core, False)

    sel_lane = lax.broadcasted_iota(jnp.int32, (16, width), 1)
    sel_row = lax.broadcasted_iota(jnp.int32, (16, width), 0)
    select = (sel_lane == jnp.where(sel_row < 8, 0, width // 2)).astype(f32).astype(bf16)
    factor = width ** (-0.5)
    queries_here, keys_here = vis_ref.shape

    def rows_of(t):
        return pl.ds(pl.multiple_of(t * 8, 8), 8)

    def score(t):
        rows = rows_of(t)
        key = kp[:, rows, :].reshape(keys_here, width).astype(bf16)
        extra = xp[:, rows, :].reshape(keys_here, width).astype(bf16)
        query = qp[:, rows, :].reshape(queries_here, width).astype(bf16)
        nt = (((1,), (1,)), ((), ()))
        scale = lax.dot_general(select, extra, nt, preferred_element_type=f32)
        scores = lax.dot_general(query, key, nt, preferred_element_type=f32)
        scores = scores * (scale[0:1] * factor)
        visible = vis_ref[...] * scale[0:1] > 0
        scores = jnp.where(visible, scores, f32(-1e30))
        highest = jnp.max(scores, axis=1, keepdims=True)
        unnormed = jnp.where(visible, jnp.exp(scores - highest), f32(0.0))
        denominator = jnp.sum(unnormed, axis=1, keepdims=True)
        held[t] = (unnormed * scale[8:9]).astype(bf16)
        safe = jnp.where(denominator > 0, denominator, f32(1.0))
        op[:, rows, :] = jnp.broadcast_to(safe, (queries_here, width)).reshape(
            queries_here // 8, 8, width
        )

    def weigh(t):
        rows = rows_of(t)
        value = vp[:, rows, :].reshape(keys_here, width).astype(bf16)
        numerator = jnp.dot(held[t], value, preferred_element_type=f32)
        result = numerator / op[:, rows, :].reshape(queries_here, width)
        op[:, rows, :] = result.astype(bf16).astype(f32).reshape(queries_here // 8, 8, width)

    groups = slots // 8
    step = groups // chips

    def score_some(d):
        for u in range(step):
            score(d * step + u)

    score_some(0)
    place_value(2 * chip + core)

    @pl.loop(1, chips)
    def _(d):
        score_some(d)
        outgoing_value(d).wait_recv()
        forward(d, *by_values).start()
        place_value(2 * source(d) + core)

        @pl.when(d == 1)
        def _():
            own_forward(*by_values).wait_recv()

        @pl.when(d > 1)
        def _():
            forward(d - 1, *by_values).wait_recv()

        place_value(2 * source(d - 1) + 1 - core)

    forward(chips - 1, *by_values).wait_recv()
    place_value(2 * source(chips - 1) + 1 - core)

    @pl.loop(0, groups // UNROLL)
    def _(t):
        for u in range(UNROLL):
            weigh(t * UNROLL + u)

    eye = (
        lax.broadcasted_iota(jnp.int32, (tok, tok), 0)
        == lax.broadcasted_iota(jnp.int32, (tok, tok), 1)
    ).astype(f32).astype(bf16)

    def answer(other):
        columns = lax.dot_general(
            eye,
            aux_of(2 * other + core).astype(bf16),
            (((1,), (1,)), ((), ())),
            preferred_element_type=f32,
        )
        slot = (columns[:, 2:3] + columns[:, 3:4]).astype(jnp.int32)
        hit = lax.broadcasted_iota(jnp.int32, (tok, slots), 1) == slot
        one = jnp.where(hit, f32(1.0), f32(0.0)).astype(bf16)
        return jnp.dot(one, op[other].astype(bf16), preferred_element_type=f32).astype(bf16)

    def reply(d):
        other = (chip + d) % chips
        return copy(ans.at[other], o_ref.at[chip], bsend.at[d], brecv.at[d], at(other))

    @pl.loop(1, chips)
    def _(d):
        other = (chip + d) % chips
        ans[other] = answer(other)

        @pl.when(d > 1)
        def _():
            reply(d - 1).start()

    o_ref[chip] = answer(chip)
    reply(chips - 1).start()
    own_forward(*by_keys).wait_send()
    own_forward(*by_values).wait_send()

    @pl.loop(1, chips)
    def _(d):
        outgoing(d).wait_send()
        outgoing_value(d).wait_send()
        forward(d, *by_keys).wait_send()
        forward(d, *by_values).wait_send()
        reply(d).wait()


def by_head(queries, key_rows, value_rows, key_scale, value_scale, cluster_label):
    tok, heads, width = queries.shape
    half = lax.axis_size("inner") // 2
    chips = lax.axis_size("outer") * half
    clusters = COARSE * FINE
    capacity = max(2, 2 * tok // clusters)
    slots = clusters * capacity
    labels = cluster_label[:, :, 0]
    earlier = jnp.arange(tok)[None, :] < jnp.arange(tok)[:, None]
    rank = jnp.sum(
        ((labels[:, :, None] == labels[:, None, :]) & earlier[None]).astype(jnp.int32), axis=2
    )
    aux = jnp.stack(
        [
            key_scale.T,
            value_scale.T,
            (labels * capacity).astype(jnp.bfloat16),
            rank.astype(jnp.bfloat16),
        ],
        axis=1,
    )
    aux = jnp.pad(aux, ((0, 0), (0, AUX - 4), (0, 0)))
    aux = aux.reshape(heads, AUX, tok // width, width).swapaxes(1, 2).reshape(heads, -1, width)
    packed = jnp.concatenate(
        [
            queries.swapaxes(0, 1),
            key_rows.swapaxes(0, 1),
            aux,
            value_rows.swapaxes(0, 1),
        ],
        axis=1,
    )
    vm = pl.BlockSpec(memory_space=pltpu.VMEM)
    dma = pltpu.SemaphoreType.DMA
    f32 = jnp.float32
    returned = pl.pallas_call(
        lambda *refs: exchange_kernel(chips, half, tok, slots, *refs),
        out_shape=jax.ShapeDtypeStruct((heads, tok, width), jnp.bfloat16),
        in_specs=[vm],
        out_specs=vm,
        scratch_shapes=[
            pltpu.VMEM((2 * chips,) + packed.shape[1:], jnp.bfloat16),
            pltpu.VMEM((chips, tok, width), jnp.bfloat16),
            pltpu.VMEM((2 * chips, slots, width), f32),
            pltpu.VMEM((2 * chips, slots, width), f32),
            pltpu.VMEM((2 * chips, slots, width), f32),
            pltpu.VMEM((chips, slots, width), f32),
            pltpu.VMEM((chips, slots, width), f32),
            pltpu.VMEM((slots // 8, 8 * chips, 16 * chips), jnp.bfloat16),
            pltpu.VMEM((8 * chips, 16 * chips), f32),
        ]
        + [dma((chips,))] * 10,
        compiler_params=pltpu.CompilerParams(
            collective_id=0, has_side_effects=True, vmem_limit_bytes=62 * 1024 * 1024
        ),
        name="clustered",
    )(packed)
    return returned.swapaxes(0, 1)


UNROLL = 4


def route(queries, key_rows, value_rows, key_scale, value_scale, cluster_label):
    tok, heads, width = queries.shape
    devices = lax.axis_size("outer") * lax.axis_size("inner")
    even = lax.axis_size("inner") % 2 == 0 and tok == 2 * width
    if devices == 2 * heads and even and 2 * tok == 4 * COARSE * FINE:
        return by_head(queries, key_rows, value_rows, key_scale, value_scale, cluster_label)
    return shards(queries, key_rows, value_rows, key_scale, value_scale, cluster_label)


def solution(mesh):
    placed = (
        P(("outer", "inner"), None, None),
        P(("outer", "inner"), None, None),
        P(("outer", "inner"), None, None),
        P(("outer", "inner"), None),
        P(("outer", "inner"), None),
        P(None, ("outer", "inner"), None),
    )
    return jax.shard_map(
        route,
        mesh=mesh,
        in_specs=placed,
        out_specs=P(("outer", "inner"), None, None),
        check_vma=False,
    )
```

```python
import jax
import jax.numpy as jnp
from jax import lax
from jax.experimental import pallas as pl
from jax.experimental.pallas import tpu as pltpu
from jax.sharding import PartitionSpec as P

COARSE = 16
FINE = 8


def attend(query_block, key_block, value_block, key_factor, value_factor, position):
    factor = query_block.shape[-1] ** (-0.5)
    scores = jnp.dot(query_block, key_block.T, preferred_element_type=jnp.float32)
    scores = scores * (key_factor.astype(jnp.float32) * factor)[None, :]
    visible = (position[None, :] >= 0) & (position[None, :] <= position[:, None])
    highest = jnp.max(jnp.where(visible, scores, jnp.float32(-1e30)), axis=1, keepdims=True)
    unnormed = jnp.where(visible, jnp.exp(scores - highest), jnp.float32(0.0))
    denominator = jnp.sum(unnormed, axis=1)
    weights = (unnormed * value_factor.astype(jnp.float32)[None, :]).astype(jnp.bfloat16)
    numerator = jnp.dot(weights, value_block, preferred_element_type=jnp.float32)
    safe = jnp.where(denominator > 0, denominator, jnp.float32(1.0))
    return (numerator / safe[:, None]).astype(jnp.bfloat16)


def attend_items(query_part, key_part, value_part, key_factor, value_factor, position):
    leading = query_part.shape[:3]
    slots = query_part.shape[3]
    width = query_part.shape[4]
    total = leading[0] * leading[1] * leading[2]

    def single(inputs):
        return attend(*inputs)

    results = lax.map(
        single,
        (
            query_part.reshape(total, slots, width),
            key_part.reshape(total, slots, width),
            value_part.reshape(total, slots, width),
            key_factor.reshape(total, slots),
            value_factor.reshape(total, slots),
            position.reshape(total, slots),
        ),
    )
    return results.reshape(leading + (slots, width))


def shards(queries, key_rows, value_rows, key_scale, value_scale, cluster_label):
    outer_count = lax.axis_size("outer")
    inner_count = lax.axis_size("inner")
    tok_rows, heads, width = queries.shape
    cluster_count = COARSE * FINE
    capacity = max(2, 2 * tok_rows // cluster_count)
    labels = cluster_label[:, :, 0].T
    member = (
        labels[:, :, None] == jnp.arange(cluster_count, dtype=jnp.int32)[None, None, :]
    ).astype(jnp.int32)
    rank = jnp.sum(jnp.cumsum(member, axis=0) * member, axis=2) - 1
    slot = (labels * heads + jnp.arange(heads, dtype=jnp.int32)[None, :]) * capacity + rank
    flat = slot.reshape(-1)
    total = cluster_count * heads * capacity
    item_count = cluster_count * heads // (outer_count * inner_count)
    layout = (outer_count, inner_count, item_count, capacity)
    source = (
        jnp.full((total,), -1, jnp.int32)
        .at[flat]
        .set(jnp.arange(tok_rows * heads, dtype=jnp.int32))
    )
    filled_slot = source >= 0
    source_row = jnp.maximum(source, 0)

    def place(array):
        rows = array.reshape((tok_rows * heads,) + array.shape[2:])
        picked = rows[source_row]
        mask = filled_slot.reshape((total,) + (1,) * (picked.ndim - 1))
        kept = jnp.where(mask, picked, jnp.zeros((), array.dtype))
        return kept.reshape(layout + array.shape[2:])

    device = lax.axis_index("outer") * inner_count + lax.axis_index("inner")
    position_rows = jnp.where(filled_slot, device * tok_rows + source_row // heads, -1).reshape(
        layout
    )
    outgoing = (
        place(queries),
        place(key_rows),
        place(value_rows),
        place(key_scale),
        place(value_scale),
        position_rows,
    )
    arrived = (
        lax.all_to_all(
            lax.all_to_all(outgoing[0], "outer", split_axis=0, concat_axis=3, tiled=True),
            "inner",
            split_axis=1,
            concat_axis=3,
            tiled=True,
        ),
        lax.all_to_all(
            lax.all_to_all(outgoing[1], "outer", split_axis=0, concat_axis=3, tiled=True),
            "inner",
            split_axis=1,
            concat_axis=3,
            tiled=True,
        ),
        lax.all_to_all(
            lax.all_to_all(outgoing[2], "outer", split_axis=0, concat_axis=3, tiled=True),
            "inner",
            split_axis=1,
            concat_axis=3,
            tiled=True,
        ),
        lax.all_to_all(
            lax.all_to_all(outgoing[3], "outer", split_axis=0, concat_axis=3, tiled=True),
            "inner",
            split_axis=1,
            concat_axis=3,
            tiled=True,
        ),
        lax.all_to_all(
            lax.all_to_all(outgoing[4], "outer", split_axis=0, concat_axis=3, tiled=True),
            "inner",
            split_axis=1,
            concat_axis=3,
            tiled=True,
        ),
        lax.all_to_all(
            lax.all_to_all(outgoing[5], "outer", split_axis=0, concat_axis=3, tiled=True),
            "inner",
            split_axis=1,
            concat_axis=3,
            tiled=True,
        ),
    )
    answered = attend_items(*arrived)
    returned = lax.all_to_all(
        lax.all_to_all(answered, "inner", split_axis=3, concat_axis=1, tiled=True),
        "outer",
        split_axis=3,
        concat_axis=0,
        tiled=True,
    )
    rows_back = returned.reshape(total, width)
    return rows_back[flat].reshape(tok_rows, heads, width)

AUX = 8


def exchange_kernel(
    chips, half, tok, slots, x_ref, o_ref, recv, ans, kp, vp, xp, qp, op, kb, vb, scales, vis_ref,
    send_sem, recv_sem, fsend, frecv, qsend, qrecv, bsend, brecv,
):
    f32, bf16 = jnp.float32, jnp.bfloat16
    width = x_ref.shape[2]
    inner = lax.axis_index("inner")
    chip = lax.axis_index("outer") * half + inner // 2
    core = inner % 2
    partner = {"outer": lax.axis_index("outer"), "inner": inner + 1 - 2 * core}
    first = x_ref.shape[1] - tok
    first_rows, query_rows = pl.ds(0, first), pl.ds(first, tok)

    def at(other):
        return {"outer": other // half, "inner": (other % half) * 2 + core}

    def copy(src, dst, s1, s2, where):
        return pltpu.make_async_remote_copy(
            src_ref=src, dst_ref=dst, send_sem=s1, recv_sem=s2,
            device_id=where, device_id_type=pl.DeviceIdType.MESH,
        )

    barrier = pltpu.get_barrier_semaphore()

    @pl.loop(1, chips)
    def _(d):
        pl.semaphore_signal(
            barrier, inc=1, device_id=at((chip + d) % chips),
            device_id_type=pl.DeviceIdType.MESH,
        )

    pl.semaphore_signal(
        barrier, inc=1, device_id=partner, device_id_type=pl.DeviceIdType.MESH
    )
    pl.semaphore_wait(barrier, chips)

    def outgoing(d):
        other = chip ^ d
        return copy(
            x_ref.at[other, first_rows], recv.at[2 * chip + core, first_rows],
            send_sem.at[d], recv_sem.at[d], at(other),
        )

    def outgoing_query(d):
        other = chip ^ d
        return copy(
            x_ref.at[other, query_rows], recv.at[2 * chip + core, query_rows],
            qsend.at[d], qrecv.at[d], at(other),
        )

    @pl.loop(1, chips)
    def _(d):
        outgoing(d).start()

    @pl.loop(1, chips)
    def _(d):
        outgoing_query(d).start()

    def own_forward():
        return copy(
            x_ref.at[chip, first_rows], recv.at[2 * chip + core, first_rows],
            fsend.at[0], frecv.at[0], partner,
        )

    def forward(d):
        row = 2 * (chip ^ d) + core
        return copy(
            recv.at[row, first_rows], recv.at[row, first_rows], fsend.at[d], frecv.at[d], partner
        )

    own_forward().start()
    recv[2 * chip + core] = x_ref[chip]

    lane = lax.broadcasted_iota(jnp.int32, (tok, width), 1)
    low = (lane < width // 2).astype(f32).astype(bf16)
    high = (lane >= width // 2).astype(f32).astype(bf16)
    key_at = lax.broadcasted_iota(jnp.int32, vis_ref.shape, 1)
    query_at = lax.broadcasted_iota(jnp.int32, vis_ref.shape, 0)
    key_order = (key_at // 8) * 4 + key_at % 4
    query_order = (2 * (query_at // 8) + core) * 4 + query_at % 4
    same = (key_at // 4) % 2 == (query_at // 4) % 2
    vis_ref[...] = jnp.where(same & (key_order <= query_order), f32(1.0), f32(0.0))
    halves = tok // width

    def aux_of(row):
        block = recv[row, pl.ds(2 * tok, AUX * halves)].astype(f32)
        return jnp.concatenate(
            [block[AUX * i : AUX * (i + 1)] for i in range(halves)], axis=1
        )

    def hits(aux):
        slot = (aux[2:3] + aux[3:4]).astype(jnp.int32)
        return lax.broadcasted_iota(jnp.int32, (slots, tok), 0) == slot

    def one_hot(hit):
        return jnp.where(hit, f32(1.0), f32(0.0)).astype(bf16)

    def place(row):
        aux = aux_of(row)
        hit = hits(aux)
        one = one_hot(hit)
        by_key = jnp.where(hit, aux[0:1], f32(0.0)).astype(bf16)
        by_value = jnp.where(hit, aux[1:2], f32(0.0)).astype(bf16)
        kp[row] = jnp.dot(one, recv[row, pl.ds(0, tok)], preferred_element_type=f32)
        vp[row] = jnp.dot(one, recv[row, pl.ds(tok, tok)], preferred_element_type=f32)
        xp[row] = jnp.dot(by_key, low, preferred_element_type=f32) + jnp.dot(
            by_value, high, preferred_element_type=f32
        )

    def place_query(other):
        row = 2 * other + core
        qp[other] = jnp.dot(
            one_hot(hits(aux_of(row))), recv[row, query_rows], preferred_element_type=f32
        )

    place(2 * chip + core)

    @pl.loop(1, chips)
    def _(d):
        outgoing(d).wait_recv()
        forward(d).start()
        place(2 * (chip ^ d) + core)

        @pl.when(d == 1)
        def _():
            own_forward().wait_recv()

        @pl.when(d > 1)
        def _():
            forward(d - 1).wait_recv()

        place(2 * (chip ^ (d - 1)) + 1 - core)

    forward(chips - 1).wait_recv()
    place(2 * (chip ^ (chips - 1)) + 1 - core)

    sel_lane = lax.broadcasted_iota(jnp.int32, (16, width), 1)
    sel_row = lax.broadcasted_iota(jnp.int32, (16, width), 0)
    select = (sel_lane == jnp.where(sel_row < 8, 0, width // 2)).astype(f32).astype(bf16)
    factor = width ** (-0.5)
    keys_here = vis_ref.shape[1]
    chunk_rows = CHUNK * 8
    nt = (((1,), (1,)), ((), ()))

    def rows_of(t):
        return pl.ds(pl.multiple_of(t * 8, 8), 8)

    @pl.loop(0, slots // 8 // UNROLL)
    def _(at_group):
        for u in range(UNROLL):
            t = at_group * UNROLL + u
            rows = rows_of(t)
            kb[t] = kp[:, rows, :].reshape(keys_here, width).astype(bf16)
            vb[t] = vp[:, rows, :].reshape(keys_here, width).astype(bf16)
            extra = xp[:, rows, :].reshape(keys_here, width).astype(bf16)
            scales[t] = lax.dot_general(select, extra, nt, preferred_element_type=f32)

    def group(base, t):
        here, rows = pl.ds(base, CHUNK), rows_of(t)
        scale = scales[t]
        query = qp[here, rows, :].reshape(chunk_rows, width).astype(bf16)
        scores = lax.dot_general(query, kb[t], nt, preferred_element_type=f32)
        scores = scores * (scale[0:1] * factor)
        allowed = vis_ref[pl.ds(pl.multiple_of(base * 8, chunk_rows), chunk_rows), :]
        visible = allowed * scale[0:1] > 0
        scores = jnp.where(visible, scores, f32(-1e30))
        highest = jnp.max(scores, axis=1, keepdims=True)
        unnormed = jnp.where(visible, jnp.exp(scores - highest), f32(0.0))
        denominator = jnp.sum(unnormed, axis=1, keepdims=True)
        weights = (unnormed * scale[8:9]).astype(bf16)
        numerator = jnp.dot(weights, vb[t], preferred_element_type=f32)
        safe = jnp.where(denominator > 0, denominator, f32(1.0))
        result = (numerator / safe).astype(bf16).astype(f32)
        op[here, rows, :] = result.reshape(CHUNK, 8, width)

    eye = (
        lax.broadcasted_iota(jnp.int32, (tok, tok), 0)
        == lax.broadcasted_iota(jnp.int32, (tok, tok), 1)
    ).astype(f32).astype(bf16)

    def answer(other):
        columns = lax.dot_general(
            eye,
            aux_of(2 * other + core).astype(bf16),
            (((1,), (1,)), ((), ())),
            preferred_element_type=f32,
        )
        slot = (columns[:, 2:3] + columns[:, 3:4]).astype(jnp.int32)
        hit = lax.broadcasted_iota(jnp.int32, (tok, slots), 1) == slot
        one = jnp.where(hit, f32(1.0), f32(0.0)).astype(bf16)
        return jnp.dot(one, op[other].astype(bf16), preferred_element_type=f32).astype(bf16)

    def reply(d):
        other = chip ^ d
        return copy(ans.at[other], o_ref.at[chip], bsend.at[d], brecv.at[d], at(other))

    def finish(first_d, last_d):
        @pl.loop(first_d, last_d)
        def _(d):
            other = chip ^ d
            ans[other] = answer(other)

            @pl.when(d > first_d)
            def _():
                reply(d - 1).start()

        reply(last_d - 1).start()

    place_query(chip)
    for part in range(chips // CHUNK):
        first_d = part * CHUNK

        @pl.loop(max(first_d, 1), first_d + CHUNK)
        def _(d):
            outgoing_query(d).wait_recv()
            place_query(chip ^ d)

        base = (chip // CHUNK ^ part) * CHUNK

        @pl.loop(0, slots // 8 // UNROLL)
        def _(at_group):
            for u in range(UNROLL):
                group(base, at_group * UNROLL + u)

        finish(max(first_d, 1), first_d + CHUNK)

    o_ref[chip] = answer(chip)
    own_forward().wait_send()

    @pl.loop(1, chips)
    def _(d):
        outgoing(d).wait_send()
        outgoing_query(d).wait_send()
        forward(d).wait_send()
        reply(d).wait()


def by_head(queries, key_rows, value_rows, key_scale, value_scale, cluster_label):
    tok, heads, width = queries.shape
    half = lax.axis_size("inner") // 2
    chips = lax.axis_size("outer") * half
    clusters = COARSE * FINE
    capacity = max(2, 2 * tok // clusters)
    slots = clusters * capacity
    labels = cluster_label[:, :, 0]
    earlier = jnp.arange(tok)[None, :] < jnp.arange(tok)[:, None]
    rank = jnp.sum(
        ((labels[:, :, None] == labels[:, None, :]) & earlier[None]).astype(jnp.int32), axis=2
    )
    aux = jnp.stack(
        [
            key_scale.T,
            value_scale.T,
            (labels * capacity).astype(jnp.bfloat16),
            rank.astype(jnp.bfloat16),
        ],
        axis=1,
    )
    aux = jnp.pad(aux, ((0, 0), (0, AUX - 4), (0, 0)))
    aux = aux.reshape(heads, AUX, tok // width, width).swapaxes(1, 2).reshape(heads, -1, width)
    packed = jnp.concatenate(
        [
            key_rows.swapaxes(0, 1),
            value_rows.swapaxes(0, 1),
            aux,
            queries.swapaxes(0, 1),
        ],
        axis=1,
    )
    vm = pl.BlockSpec(memory_space=pltpu.VMEM)
    dma = pltpu.SemaphoreType.DMA
    f32 = jnp.float32
    returned = pl.pallas_call(
        lambda *refs: exchange_kernel(chips, half, tok, slots, *refs),
        out_shape=jax.ShapeDtypeStruct((heads, tok, width), jnp.bfloat16),
        in_specs=[vm],
        out_specs=vm,
        scratch_shapes=[
            pltpu.VMEM((2 * chips,) + packed.shape[1:], jnp.bfloat16),
            pltpu.VMEM((chips, tok, width), jnp.bfloat16),
            pltpu.VMEM((2 * chips, slots, width), f32),
            pltpu.VMEM((2 * chips, slots, width), f32),
            pltpu.VMEM((2 * chips, slots, width), f32),
            pltpu.VMEM((chips, slots, width), f32),
            pltpu.VMEM((chips, slots, width), f32),
            pltpu.VMEM((slots // 8, 16 * chips, width), jnp.bfloat16),
            pltpu.VMEM((slots // 8, 16 * chips, width), jnp.bfloat16),
            pltpu.VMEM((slots // 8, 16, 16 * chips), f32),
            pltpu.VMEM((8 * chips, 16 * chips), f32),
        ]
        + [dma((chips,))] * 8,
        compiler_params=pltpu.CompilerParams(
            collective_id=0, has_side_effects=True, vmem_limit_bytes=62 * 1024 * 1024
        ),
        name="clustered",
    )(packed)
    return returned.swapaxes(0, 1)


UNROLL = 4
CHUNK = 4


def route(queries, key_rows, value_rows, key_scale, value_scale, cluster_label):
    tok, heads, width = queries.shape
    devices = lax.axis_size("outer") * lax.axis_size("inner")
    even = lax.axis_size("inner") % 2 == 0 and tok == 2 * width
    even = even and heads & (heads - 1) == 0 and heads % CHUNK == 0
    if devices == 2 * heads and even and 2 * tok == 4 * COARSE * FINE:
        return by_head(queries, key_rows, value_rows, key_scale, value_scale, cluster_label)
    return shards(queries, key_rows, value_rows, key_scale, value_scale, cluster_label)


def solution(mesh):
    placed = (
        P(("outer", "inner"), None, None),
        P(("outer", "inner"), None, None),
        P(("outer", "inner"), None, None),
        P(("outer", "inner"), None),
        P(("outer", "inner"), None),
        P(None, ("outer", "inner"), None),
    )
    return jax.shard_map(
        route,
        mesh=mesh,
        in_specs=placed,
        out_specs=P(("outer", "inner"), None, None),
        check_vma=False,
    )
```

```python
import jax
import jax.numpy as jnp
from jax import lax
from jax.experimental import pallas as pl
from jax.experimental.pallas import tpu as pltpu
from jax.sharding import PartitionSpec as P

COARSE = 16
FINE = 8


def attend(query_block, key_block, value_block, key_factor, value_factor, position):
    factor = query_block.shape[-1] ** (-0.5)
    scores = jnp.dot(query_block, key_block.T, preferred_element_type=jnp.float32)
    scores = scores * (key_factor.astype(jnp.float32) * factor)[None, :]
    visible = (position[None, :] >= 0) & (position[None, :] <= position[:, None])
    highest = jnp.max(jnp.where(visible, scores, jnp.float32(-1e30)), axis=1, keepdims=True)
    unnormed = jnp.where(visible, jnp.exp(scores - highest), jnp.float32(0.0))
    denominator = jnp.sum(unnormed, axis=1)
    weights = (unnormed * value_factor.astype(jnp.float32)[None, :]).astype(jnp.bfloat16)
    numerator = jnp.dot(weights, value_block, preferred_element_type=jnp.float32)
    safe = jnp.where(denominator > 0, denominator, jnp.float32(1.0))
    return (numerator / safe[:, None]).astype(jnp.bfloat16)


def attend_items(query_part, key_part, value_part, key_factor, value_factor, position):
    leading = query_part.shape[:3]
    slots = query_part.shape[3]
    width = query_part.shape[4]
    total = leading[0] * leading[1] * leading[2]

    def single(inputs):
        return attend(*inputs)

    results = lax.map(
        single,
        (
            query_part.reshape(total, slots, width),
            key_part.reshape(total, slots, width),
            value_part.reshape(total, slots, width),
            key_factor.reshape(total, slots),
            value_factor.reshape(total, slots),
            position.reshape(total, slots),
        ),
    )
    return results.reshape(leading + (slots, width))


def shards(queries, key_rows, value_rows, key_scale, value_scale, cluster_label):
    outer_count = lax.axis_size("outer")
    inner_count = lax.axis_size("inner")
    tok_rows, heads, width = queries.shape
    cluster_count = COARSE * FINE
    capacity = max(2, 2 * tok_rows // cluster_count)
    labels = cluster_label[:, :, 0].T
    member = (
        labels[:, :, None] == jnp.arange(cluster_count, dtype=jnp.int32)[None, None, :]
    ).astype(jnp.int32)
    rank = jnp.sum(jnp.cumsum(member, axis=0) * member, axis=2) - 1
    slot = (labels * heads + jnp.arange(heads, dtype=jnp.int32)[None, :]) * capacity + rank
    flat = slot.reshape(-1)
    total = cluster_count * heads * capacity
    item_count = cluster_count * heads // (outer_count * inner_count)
    layout = (outer_count, inner_count, item_count, capacity)
    source = (
        jnp.full((total,), -1, jnp.int32)
        .at[flat]
        .set(jnp.arange(tok_rows * heads, dtype=jnp.int32))
    )
    filled_slot = source >= 0
    source_row = jnp.maximum(source, 0)

    def place(array):
        rows = array.reshape((tok_rows * heads,) + array.shape[2:])
        picked = rows[source_row]
        mask = filled_slot.reshape((total,) + (1,) * (picked.ndim - 1))
        kept = jnp.where(mask, picked, jnp.zeros((), array.dtype))
        return kept.reshape(layout + array.shape[2:])

    device = lax.axis_index("outer") * inner_count + lax.axis_index("inner")
    position_rows = jnp.where(filled_slot, device * tok_rows + source_row // heads, -1).reshape(
        layout
    )
    outgoing = (
        place(queries),
        place(key_rows),
        place(value_rows),
        place(key_scale),
        place(value_scale),
        position_rows,
    )
    arrived = (
        lax.all_to_all(
            lax.all_to_all(outgoing[0], "outer", split_axis=0, concat_axis=3, tiled=True),
            "inner",
            split_axis=1,
            concat_axis=3,
            tiled=True,
        ),
        lax.all_to_all(
            lax.all_to_all(outgoing[1], "outer", split_axis=0, concat_axis=3, tiled=True),
            "inner",
            split_axis=1,
            concat_axis=3,
            tiled=True,
        ),
        lax.all_to_all(
            lax.all_to_all(outgoing[2], "outer", split_axis=0, concat_axis=3, tiled=True),
            "inner",
            split_axis=1,
            concat_axis=3,
            tiled=True,
        ),
        lax.all_to_all(
            lax.all_to_all(outgoing[3], "outer", split_axis=0, concat_axis=3, tiled=True),
            "inner",
            split_axis=1,
            concat_axis=3,
            tiled=True,
        ),
        lax.all_to_all(
            lax.all_to_all(outgoing[4], "outer", split_axis=0, concat_axis=3, tiled=True),
            "inner",
            split_axis=1,
            concat_axis=3,
            tiled=True,
        ),
        lax.all_to_all(
            lax.all_to_all(outgoing[5], "outer", split_axis=0, concat_axis=3, tiled=True),
            "inner",
            split_axis=1,
            concat_axis=3,
            tiled=True,
        ),
    )
    answered = attend_items(*arrived)
    returned = lax.all_to_all(
        lax.all_to_all(answered, "inner", split_axis=3, concat_axis=1, tiled=True),
        "outer",
        split_axis=3,
        concat_axis=0,
        tiled=True,
    )
    rows_back = returned.reshape(total, width)
    return rows_back[flat].reshape(tok_rows, heads, width)

AUX = 8


def exchange_kernel(
    chips, half, tok, slots, x_ref, o_ref, recv, ans, kp, vp, xp, qp, op, kb, vb, scales, vis_ref,
    send_sem, recv_sem, fsend, frecv, qsend, qrecv, bsend, brecv,
):
    f32, bf16 = jnp.float32, jnp.bfloat16
    width = x_ref.shape[2]
    inner = lax.axis_index("inner")
    chip = lax.axis_index("outer") * half + inner // 2
    core = inner % 2
    partner = {"outer": lax.axis_index("outer"), "inner": inner + 1 - 2 * core}
    first = x_ref.shape[1] - tok
    first_rows, query_rows = pl.ds(0, first), pl.ds(first, tok)

    def at(other):
        return {"outer": other // half, "inner": (other % half) * 2 + core}

    def copy(src, dst, s1, s2, where):
        return pltpu.make_async_remote_copy(
            src_ref=src, dst_ref=dst, send_sem=s1, recv_sem=s2,
            device_id=where, device_id_type=pl.DeviceIdType.MESH,
        )

    barrier = pltpu.get_barrier_semaphore()

    @pl.loop(1, chips)
    def _(d):
        pl.semaphore_signal(
            barrier, inc=1, device_id=at((chip + d) % chips),
            device_id_type=pl.DeviceIdType.MESH,
        )

    pl.semaphore_signal(
        barrier, inc=1, device_id=partner, device_id_type=pl.DeviceIdType.MESH
    )
    pl.semaphore_wait(barrier, chips)

    def outgoing(d):
        other = chip ^ d
        return copy(
            x_ref.at[other, first_rows], recv.at[2 * chip + core, first_rows],
            send_sem.at[d], recv_sem.at[d], at(other),
        )

    def outgoing_query(d):
        other = chip ^ d
        return copy(
            x_ref.at[other, query_rows], recv.at[2 * chip + core, query_rows],
            qsend.at[d], qrecv.at[d], at(other),
        )

    @pl.loop(1, chips)
    def _(d):
        outgoing(d).start()

    @pl.loop(1, chips)
    def _(d):
        outgoing_query(d).start()

    def own_forward():
        return copy(
            x_ref.at[chip, first_rows], recv.at[2 * chip + core, first_rows],
            fsend.at[0], frecv.at[0], partner,
        )

    def forward(d):
        row = 2 * (chip ^ d) + core
        return copy(
            recv.at[row, first_rows], recv.at[row, first_rows], fsend.at[d], frecv.at[d], partner
        )

    own_forward().start()
    recv[2 * chip + core] = x_ref[chip]

    lane = lax.broadcasted_iota(jnp.int32, (tok, width), 1)
    low = (lane < width // 2).astype(f32).astype(bf16)
    high = (lane >= width // 2).astype(f32).astype(bf16)
    key_at = lax.broadcasted_iota(jnp.int32, vis_ref.shape, 1)
    query_at = lax.broadcasted_iota(jnp.int32, vis_ref.shape, 0)
    key_order = (key_at // 8) * 4 + key_at % 4
    query_order = (2 * (query_at // 8) + core) * 4 + query_at % 4
    same = (key_at // 4) % 2 == (query_at // 4) % 2
    vis_ref[...] = jnp.where(same & (key_order <= query_order), f32(1.0), f32(0.0))
    halves = tok // width

    def aux_of(row):
        block = recv[row, pl.ds(2 * tok, AUX * halves)].astype(f32)
        return jnp.concatenate(
            [block[AUX * i : AUX * (i + 1)] for i in range(halves)], axis=1
        )

    def hits(aux):
        slot = (aux[2:3] + aux[3:4]).astype(jnp.int32)
        return lax.broadcasted_iota(jnp.int32, (slots, tok), 0) == slot

    def one_hot(hit):
        return jnp.where(hit, f32(1.0), f32(0.0)).astype(bf16)

    def place(row):
        aux = aux_of(row)
        hit = hits(aux)
        one = one_hot(hit)
        by_key = jnp.where(hit, aux[0:1], f32(0.0)).astype(bf16)
        by_value = jnp.where(hit, aux[1:2], f32(0.0)).astype(bf16)
        kp[row] = jnp.dot(one, recv[row, pl.ds(0, tok)], preferred_element_type=f32)
        vp[row] = jnp.dot(one, recv[row, pl.ds(tok, tok)], preferred_element_type=f32)
        xp[row] = jnp.dot(by_key, low, preferred_element_type=f32) + jnp.dot(
            by_value, high, preferred_element_type=f32
        )

    def place_query(other):
        row = 2 * other + core
        qp[other] = jnp.dot(
            one_hot(hits(aux_of(row))), recv[row, query_rows], preferred_element_type=f32
        )

    place(2 * chip + core)

    @pl.loop(1, chips)
    def _(d):
        outgoing(d).wait_recv()
        forward(d).start()
        place(2 * (chip ^ d) + core)

        @pl.when(d == 1)
        def _():
            own_forward().wait_recv()

        @pl.when(d > 1)
        def _():
            forward(d - 1).wait_recv()

        place(2 * (chip ^ (d - 1)) + 1 - core)

    forward(chips - 1).wait_recv()
    place(2 * (chip ^ (chips - 1)) + 1 - core)

    sel_lane = lax.broadcasted_iota(jnp.int32, (16, width), 1)
    sel_row = lax.broadcasted_iota(jnp.int32, (16, width), 0)
    select = (sel_lane == jnp.where(sel_row < 8, 0, width // 2)).astype(f32).astype(bf16)
    factor = width ** (-0.5)
    keys_here = vis_ref.shape[1]
    chunk_rows = CHUNK * 8
    nt = (((1,), (1,)), ((), ()))

    def rows_of(t):
        return pl.ds(pl.multiple_of(t * 8, 8), 8)

    @pl.loop(0, slots // 8 // UNROLL)
    def _(at_group):
        for u in range(UNROLL):
            t = at_group * UNROLL + u
            rows = rows_of(t)
            kb[t] = kp[:, rows, :].reshape(keys_here, width).astype(bf16)
            vb[t] = vp[:, rows, :].reshape(keys_here, width).astype(bf16)
            extra = xp[:, rows, :].reshape(keys_here, width).astype(bf16)
            scales[t] = lax.dot_general(select, extra, nt, preferred_element_type=f32)

    def attend_groups(base, groups):
        here = pl.ds(base, CHUNK)
        allowed = vis_ref[pl.ds(pl.multiple_of(base * 8, chunk_rows), chunk_rows), :]
        scale = [scales[t] for t in groups]
        query = [qp[here, rows_of(t), :].reshape(chunk_rows, width).astype(bf16) for t in groups]
        scores = [
            lax.dot_general(q, kb[t], nt, preferred_element_type=f32)
            for q, t in zip(query, groups)
        ]
        visible = [allowed * c[0:1] > 0 for c in scale]
        scores = [
            jnp.where(ok, s * (c[0:1] * factor), f32(-1e30))
            for ok, s, c in zip(visible, scores, scale)
        ]
        highest = [jnp.max(s, axis=1, keepdims=True) for s in scores]
        unnormed = [
            jnp.where(ok, jnp.exp(s - m), f32(0.0))
            for ok, s, m in zip(visible, scores, highest)
        ]
        weights = [(e * c[8:9]).astype(bf16) for e, c in zip(unnormed, scale)]
        numerator = [
            jnp.dot(w, vb[t], preferred_element_type=f32) for w, t in zip(weights, groups)
        ]
        denominator = [jnp.sum(e, axis=1, keepdims=True) for e in unnormed]
        safe = [jnp.where(n > 0, n, f32(1.0)) for n in denominator]
        result = [(n / d).astype(bf16).astype(f32) for n, d in zip(numerator, safe)]
        for r, t in zip(result, groups):
            op[here, rows_of(t), :] = r.reshape(CHUNK, 8, width)

    eye = (
        lax.broadcasted_iota(jnp.int32, (tok, tok), 0)
        == lax.broadcasted_iota(jnp.int32, (tok, tok), 1)
    ).astype(f32).astype(bf16)

    def answer(other):
        columns = lax.dot_general(
            eye,
            aux_of(2 * other + core).astype(bf16),
            (((1,), (1,)), ((), ())),
            preferred_element_type=f32,
        )
        slot = (columns[:, 2:3] + columns[:, 3:4]).astype(jnp.int32)
        hit = lax.broadcasted_iota(jnp.int32, (tok, slots), 1) == slot
        one = jnp.where(hit, f32(1.0), f32(0.0)).astype(bf16)
        return jnp.dot(one, op[other].astype(bf16), preferred_element_type=f32).astype(bf16)

    def reply(d):
        other = chip ^ d
        return copy(ans.at[other], o_ref.at[chip], bsend.at[d], brecv.at[d], at(other))

    def finish(first_d, last_d):
        @pl.loop(first_d, last_d)
        def _(d):
            other = chip ^ d
            ans[other] = answer(other)

            @pl.when(d > first_d)
            def _():
                reply(d - 1).start()

        reply(last_d - 1).start()

    place_query(chip)
    for part in range(chips // CHUNK):
        first_d = part * CHUNK

        @pl.loop(max(first_d, 1), first_d + CHUNK)
        def _(d):
            outgoing_query(d).wait_recv()
            place_query(chip ^ d)

        base = (chip // CHUNK ^ part) * CHUNK

        @pl.loop(0, slots // 8 // UNROLL)
        def _(at_group):
            attend_groups(base, [at_group * UNROLL + u for u in range(UNROLL)])

        finish(max(first_d, 1), first_d + CHUNK)

    o_ref[chip] = answer(chip)
    own_forward().wait_send()

    @pl.loop(1, chips)
    def _(d):
        outgoing(d).wait_send()
        outgoing_query(d).wait_send()
        forward(d).wait_send()
        reply(d).wait()


def by_head(queries, key_rows, value_rows, key_scale, value_scale, cluster_label):
    tok, heads, width = queries.shape
    half = lax.axis_size("inner") // 2
    chips = lax.axis_size("outer") * half
    clusters = COARSE * FINE
    capacity = max(2, 2 * tok // clusters)
    slots = clusters * capacity
    labels = cluster_label[:, :, 0]
    earlier = jnp.arange(tok)[None, :] < jnp.arange(tok)[:, None]
    rank = jnp.sum(
        ((labels[:, :, None] == labels[:, None, :]) & earlier[None]).astype(jnp.int32), axis=2
    )
    aux = jnp.stack(
        [
            key_scale.T,
            value_scale.T,
            (labels * capacity).astype(jnp.bfloat16),
            rank.astype(jnp.bfloat16),
        ],
        axis=1,
    )
    aux = jnp.pad(aux, ((0, 0), (0, AUX - 4), (0, 0)))
    aux = aux.reshape(heads, AUX, tok // width, width).swapaxes(1, 2).reshape(heads, -1, width)
    packed = jnp.concatenate(
        [
            key_rows.swapaxes(0, 1),
            value_rows.swapaxes(0, 1),
            aux,
            queries.swapaxes(0, 1),
        ],
        axis=1,
    )
    vm = pl.BlockSpec(memory_space=pltpu.VMEM)
    dma = pltpu.SemaphoreType.DMA
    f32 = jnp.float32
    returned = pl.pallas_call(
        lambda *refs: exchange_kernel(chips, half, tok, slots, *refs),
        out_shape=jax.ShapeDtypeStruct((heads, tok, width), jnp.bfloat16),
        in_specs=[vm],
        out_specs=vm,
        scratch_shapes=[
            pltpu.VMEM((2 * chips,) + packed.shape[1:], jnp.bfloat16),
            pltpu.VMEM((chips, tok, width), jnp.bfloat16),
            pltpu.VMEM((2 * chips, slots, width), f32),
            pltpu.VMEM((2 * chips, slots, width), f32),
            pltpu.VMEM((2 * chips, slots, width), f32),
            pltpu.VMEM((chips, slots, width), f32),
            pltpu.VMEM((chips, slots, width), f32),
            pltpu.VMEM((slots // 8, 16 * chips, width), jnp.bfloat16),
            pltpu.VMEM((slots // 8, 16 * chips, width), jnp.bfloat16),
            pltpu.VMEM((slots // 8, 16, 16 * chips), f32),
            pltpu.VMEM((8 * chips, 16 * chips), f32),
        ]
        + [dma((chips,))] * 8,
        compiler_params=pltpu.CompilerParams(
            collective_id=0, has_side_effects=True, vmem_limit_bytes=62 * 1024 * 1024
        ),
        name="clustered",
    )(packed)
    return returned.swapaxes(0, 1)


UNROLL = 8
CHUNK = 8


def route(queries, key_rows, value_rows, key_scale, value_scale, cluster_label):
    tok, heads, width = queries.shape
    devices = lax.axis_size("outer") * lax.axis_size("inner")
    even = lax.axis_size("inner") % 2 == 0 and tok == 2 * width
    even = even and heads & (heads - 1) == 0 and heads % CHUNK == 0
    if devices == 2 * heads and even and 2 * tok == 4 * COARSE * FINE:
        return by_head(queries, key_rows, value_rows, key_scale, value_scale, cluster_label)
    return shards(queries, key_rows, value_rows, key_scale, value_scale, cluster_label)


def solution(mesh):
    placed = (
        P(("outer", "inner"), None, None),
        P(("outer", "inner"), None, None),
        P(("outer", "inner"), None, None),
        P(("outer", "inner"), None),
        P(("outer", "inner"), None),
        P(None, ("outer", "inner"), None),
    )
    return jax.shard_map(
        route,
        mesh=mesh,
        in_specs=placed,
        out_specs=P(("outer", "inner"), None, None),
        check_vma=False,
    )
```

```python
import jax
import jax.numpy as jnp
from jax import lax
from jax.experimental import pallas as pl
from jax.experimental.pallas import tpu as pltpu
from jax.sharding import PartitionSpec as P

COARSE = 16
FINE = 8


def attend(query_block, key_block, value_block, key_factor, value_factor, position):
    factor = query_block.shape[-1] ** (-0.5)
    scores = jnp.dot(query_block, key_block.T, preferred_element_type=jnp.float32)
    scores = scores * (key_factor.astype(jnp.float32) * factor)[None, :]
    visible = (position[None, :] >= 0) & (position[None, :] <= position[:, None])
    highest = jnp.max(jnp.where(visible, scores, jnp.float32(-1e30)), axis=1, keepdims=True)
    unnormed = jnp.where(visible, jnp.exp(scores - highest), jnp.float32(0.0))
    denominator = jnp.sum(unnormed, axis=1)
    weights = (unnormed * value_factor.astype(jnp.float32)[None, :]).astype(jnp.bfloat16)
    numerator = jnp.dot(weights, value_block, preferred_element_type=jnp.float32)
    safe = jnp.where(denominator > 0, denominator, jnp.float32(1.0))
    return (numerator / safe[:, None]).astype(jnp.bfloat16)


def attend_items(query_part, key_part, value_part, key_factor, value_factor, position):
    leading = query_part.shape[:3]
    slots = query_part.shape[3]
    width = query_part.shape[4]
    total = leading[0] * leading[1] * leading[2]

    def single(inputs):
        return attend(*inputs)

    results = lax.map(
        single,
        (
            query_part.reshape(total, slots, width),
            key_part.reshape(total, slots, width),
            value_part.reshape(total, slots, width),
            key_factor.reshape(total, slots),
            value_factor.reshape(total, slots),
            position.reshape(total, slots),
        ),
    )
    return results.reshape(leading + (slots, width))


def shards(queries, key_rows, value_rows, key_scale, value_scale, cluster_label):
    outer_count = lax.axis_size("outer")
    inner_count = lax.axis_size("inner")
    tok_rows, heads, width = queries.shape
    cluster_count = COARSE * FINE
    capacity = max(2, 2 * tok_rows // cluster_count)
    labels = cluster_label[:, :, 0].T
    member = (
        labels[:, :, None] == jnp.arange(cluster_count, dtype=jnp.int32)[None, None, :]
    ).astype(jnp.int32)
    rank = jnp.sum(jnp.cumsum(member, axis=0) * member, axis=2) - 1
    slot = (labels * heads + jnp.arange(heads, dtype=jnp.int32)[None, :]) * capacity + rank
    flat = slot.reshape(-1)
    total = cluster_count * heads * capacity
    item_count = cluster_count * heads // (outer_count * inner_count)
    layout = (outer_count, inner_count, item_count, capacity)
    source = (
        jnp.full((total,), -1, jnp.int32)
        .at[flat]
        .set(jnp.arange(tok_rows * heads, dtype=jnp.int32))
    )
    filled_slot = source >= 0
    source_row = jnp.maximum(source, 0)

    def place(array):
        rows = array.reshape((tok_rows * heads,) + array.shape[2:])
        picked = rows[source_row]
        mask = filled_slot.reshape((total,) + (1,) * (picked.ndim - 1))
        kept = jnp.where(mask, picked, jnp.zeros((), array.dtype))
        return kept.reshape(layout + array.shape[2:])

    device = lax.axis_index("outer") * inner_count + lax.axis_index("inner")
    position_rows = jnp.where(filled_slot, device * tok_rows + source_row // heads, -1).reshape(
        layout
    )
    outgoing = (
        place(queries),
        place(key_rows),
        place(value_rows),
        place(key_scale),
        place(value_scale),
        position_rows,
    )
    arrived = (
        lax.all_to_all(
            lax.all_to_all(outgoing[0], "outer", split_axis=0, concat_axis=3, tiled=True),
            "inner",
            split_axis=1,
            concat_axis=3,
            tiled=True,
        ),
        lax.all_to_all(
            lax.all_to_all(outgoing[1], "outer", split_axis=0, concat_axis=3, tiled=True),
            "inner",
            split_axis=1,
            concat_axis=3,
            tiled=True,
        ),
        lax.all_to_all(
            lax.all_to_all(outgoing[2], "outer", split_axis=0, concat_axis=3, tiled=True),
            "inner",
            split_axis=1,
            concat_axis=3,
            tiled=True,
        ),
        lax.all_to_all(
            lax.all_to_all(outgoing[3], "outer", split_axis=0, concat_axis=3, tiled=True),
            "inner",
            split_axis=1,
            concat_axis=3,
            tiled=True,
        ),
        lax.all_to_all(
            lax.all_to_all(outgoing[4], "outer", split_axis=0, concat_axis=3, tiled=True),
            "inner",
            split_axis=1,
            concat_axis=3,
            tiled=True,
        ),
        lax.all_to_all(
            lax.all_to_all(outgoing[5], "outer", split_axis=0, concat_axis=3, tiled=True),
            "inner",
            split_axis=1,
            concat_axis=3,
            tiled=True,
        ),
    )
    answered = attend_items(*arrived)
    returned = lax.all_to_all(
        lax.all_to_all(answered, "inner", split_axis=3, concat_axis=1, tiled=True),
        "outer",
        split_axis=3,
        concat_axis=0,
        tiled=True,
    )
    rows_back = returned.reshape(total, width)
    return rows_back[flat].reshape(tok_rows, heads, width)

AUX = 8


def exchange_kernel(
    chips, half, tok, slots, x_ref, o_ref, recv, ans, kp, vp, xp, qp, op, kb, vb, scales, vis_ref,
    send_sem, recv_sem, fsend, frecv, qsend, qrecv, bsend, brecv,
):
    f32, bf16 = jnp.float32, jnp.bfloat16
    width = x_ref.shape[2]
    inner = lax.axis_index("inner")
    chip = lax.axis_index("outer") * half + inner // 2
    core = inner % 2
    partner = {"outer": lax.axis_index("outer"), "inner": inner + 1 - 2 * core}
    first = x_ref.shape[1] - tok
    first_rows, query_rows = pl.ds(0, first), pl.ds(first, tok)

    def at(other):
        return {"outer": other // half, "inner": (other % half) * 2 + core}

    def copy(src, dst, s1, s2, where):
        return pltpu.make_async_remote_copy(
            src_ref=src, dst_ref=dst, send_sem=s1, recv_sem=s2,
            device_id=where, device_id_type=pl.DeviceIdType.MESH,
        )

    barrier = pltpu.get_barrier_semaphore()

    @pl.loop(1, chips)
    def _(d):
        pl.semaphore_signal(
            barrier, inc=1, device_id=at((chip + d) % chips),
            device_id_type=pl.DeviceIdType.MESH,
        )

    pl.semaphore_signal(
        barrier, inc=1, device_id=partner, device_id_type=pl.DeviceIdType.MESH
    )
    pl.semaphore_wait(barrier, chips)

    def outgoing(d):
        other = chip ^ d
        return copy(
            x_ref.at[other, first_rows], recv.at[2 * chip + core, first_rows],
            send_sem.at[d], recv_sem.at[d], at(other),
        )

    def outgoing_query(d):
        other = chip ^ d
        return copy(
            x_ref.at[other, query_rows], recv.at[2 * chip + core, query_rows],
            qsend.at[d], qrecv.at[d], at(other),
        )

    @pl.loop(1, chips)
    def _(d):
        outgoing(d).start()

    @pl.loop(1, chips)
    def _(d):
        outgoing_query(d).start()

    def own_forward():
        return copy(
            x_ref.at[chip, first_rows], recv.at[2 * chip + core, first_rows],
            fsend.at[0], frecv.at[0], partner,
        )

    def forward(d):
        row = 2 * (chip ^ d) + core
        return copy(
            recv.at[row, first_rows], recv.at[row, first_rows], fsend.at[d], frecv.at[d], partner
        )

    own_forward().start()
    recv[2 * chip + core] = x_ref[chip]

    lane = lax.broadcasted_iota(jnp.int32, (tok, width), 1)
    low = (lane < width // 2).astype(f32).astype(bf16)
    high = (lane >= width // 2).astype(f32).astype(bf16)
    key_at = lax.broadcasted_iota(jnp.int32, vis_ref.shape, 1)
    query_at = lax.broadcasted_iota(jnp.int32, vis_ref.shape, 0)
    key_order = (key_at // 8) * 4 + key_at % 4
    query_order = (2 * (query_at // 8) + core) * 4 + query_at % 4
    same = (key_at // 4) % 2 == (query_at // 4) % 2
    vis_ref[...] = jnp.where(same & (key_order <= query_order), f32(1.0), f32(0.0))
    halves = tok // width

    def aux_of(row):
        block = recv[row, pl.ds(2 * tok, AUX * halves)].astype(f32)
        return jnp.concatenate(
            [block[AUX * i : AUX * (i + 1)] for i in range(halves)], axis=1
        )

    def hits(aux):
        slot = (aux[2:3] + aux[3:4]).astype(jnp.int32)
        return lax.broadcasted_iota(jnp.int32, (slots, tok), 0) == slot

    def one_hot(hit):
        return jnp.where(hit, f32(1.0), f32(0.0)).astype(bf16)

    def place(row):
        aux = aux_of(row)
        hit = hits(aux)
        one = one_hot(hit)
        by_key = jnp.where(hit, aux[0:1], f32(0.0)).astype(bf16)
        by_value = jnp.where(hit, aux[1:2], f32(0.0)).astype(bf16)
        kp[row] = jnp.dot(one, recv[row, pl.ds(0, tok)], preferred_element_type=f32)
        vp[row] = jnp.dot(one, recv[row, pl.ds(tok, tok)], preferred_element_type=f32)
        xp[row] = jnp.dot(by_key, low, preferred_element_type=f32) + jnp.dot(
            by_value, high, preferred_element_type=f32
        )

    def place_query(other):
        row = 2 * other + core
        qp[other] = jnp.dot(
            one_hot(hits(aux_of(row))), recv[row, query_rows], preferred_element_type=f32
        )

    place(2 * chip + core)

    @pl.loop(1, chips)
    def _(d):
        outgoing(d).wait_recv()
        forward(d).start()
        place(2 * (chip ^ d) + core)

        @pl.when(d == 1)
        def _():
            own_forward().wait_recv()

        @pl.when(d > 1)
        def _():
            forward(d - 1).wait_recv()

        place(2 * (chip ^ (d - 1)) + 1 - core)

    forward(chips - 1).wait_recv()
    place(2 * (chip ^ (chips - 1)) + 1 - core)

    sel_lane = lax.broadcasted_iota(jnp.int32, (16, width), 1)
    sel_row = lax.broadcasted_iota(jnp.int32, (16, width), 0)
    select = (sel_lane == jnp.where(sel_row < 8, 0, width // 2)).astype(f32).astype(bf16)
    factor = width ** (-0.5)
    keys_here = vis_ref.shape[1]
    chunk_rows = CHUNK * 8
    nt = (((1,), (1,)), ((), ()))

    def rows_of(t):
        return pl.ds(pl.multiple_of(t * 8, 8), 8)

    @pl.loop(0, slots // 8 // UNROLL)
    def _(at_group):
        for u in range(UNROLL):
            t = at_group * UNROLL + u
            rows = rows_of(t)
            kb[t] = kp[:, rows, :].reshape(keys_here, width).astype(bf16)
            vb[t] = vp[:, rows, :].reshape(keys_here, width).astype(bf16)
            extra = xp[:, rows, :].reshape(keys_here, width).astype(bf16)
            scales[t] = lax.dot_general(select, extra, nt, preferred_element_type=f32)

    def attend_groups(base, groups):
        here = pl.ds(base, CHUNK)
        allowed = vis_ref[pl.ds(pl.multiple_of(base * 8, chunk_rows), chunk_rows), :]
        scale = [scales[t] for t in groups]
        query = [qp[here, rows_of(t), :].reshape(chunk_rows, width).astype(bf16) for t in groups]
        scores = [
            lax.dot_general(q, kb[t], nt, preferred_element_type=f32)
            for q, t in zip(query, groups)
        ]
        visible = [allowed * c[0:1] > 0 for c in scale]
        scores = [
            jnp.where(ok, s * (c[0:1] * factor), f32(-1e30))
            for ok, s, c in zip(visible, scores, scale)
        ]
        highest = [jnp.max(s, axis=1, keepdims=True) for s in scores]
        unnormed = [
            jnp.where(ok, jnp.exp(s - m), f32(0.0))
            for ok, s, m in zip(visible, scores, highest)
        ]
        weights = [(e * c[8:9]).astype(bf16) for e, c in zip(unnormed, scale)]
        numerator = [
            jnp.dot(w, vb[t], preferred_element_type=f32) for w, t in zip(weights, groups)
        ]
        denominator = [jnp.sum(e, axis=1, keepdims=True) for e in unnormed]
        safe = [jnp.where(n > 0, n, f32(1.0)) for n in denominator]
        result = [(n / d).astype(bf16).astype(f32) for n, d in zip(numerator, safe)]
        for r, t in zip(result, groups):
            op[here, rows_of(t), :] = r.reshape(CHUNK, 8, width)

    eye = (
        lax.broadcasted_iota(jnp.int32, (tok, tok), 0)
        == lax.broadcasted_iota(jnp.int32, (tok, tok), 1)
    ).astype(f32).astype(bf16)

    def answer(other):
        columns = lax.dot_general(
            eye,
            aux_of(2 * other + core).astype(bf16),
            (((1,), (1,)), ((), ())),
            preferred_element_type=f32,
        )
        slot = (columns[:, 2:3] + columns[:, 3:4]).astype(jnp.int32)
        hit = lax.broadcasted_iota(jnp.int32, (tok, slots), 1) == slot
        one = jnp.where(hit, f32(1.0), f32(0.0)).astype(bf16)
        return jnp.dot(one, op[other].astype(bf16), preferred_element_type=f32).astype(bf16)

    def reply(d):
        other = chip ^ d
        return copy(ans.at[other], o_ref.at[chip], bsend.at[d], brecv.at[d], at(other))

    def finish(first_d, last_d):
        @pl.loop(first_d, last_d)
        def _(d):
            other = chip ^ d
            ans[other] = answer(other)

            @pl.when(d > first_d)
            def _():
                reply(d - 1).start()

        reply(last_d - 1).start()

    place_query(chip)
    for part in range(chips // CHUNK):
        first_d = part * CHUNK

        @pl.loop(max(first_d, 1), first_d + CHUNK)
        def _(d):
            outgoing_query(d).wait_recv()
            place_query(chip ^ d)

        base = (chip // CHUNK ^ part) * CHUNK

        @pl.loop(0, slots // 8 // UNROLL)
        def _(at_group):
            attend_groups(base, [at_group * UNROLL + u for u in range(UNROLL)])

        finish(max(first_d, 1), first_d + CHUNK)

    o_ref[chip] = answer(chip)
    own_forward().wait_send()

    @pl.loop(1, chips)
    def _(d):
        outgoing(d).wait_send()
        outgoing_query(d).wait_send()
        forward(d).wait_send()
        reply(d).wait()


def by_head(queries, key_rows, value_rows, key_scale, value_scale, cluster_label):
    tok, heads, width = queries.shape
    half = lax.axis_size("inner") // 2
    chips = lax.axis_size("outer") * half
    clusters = COARSE * FINE
    capacity = max(2, 2 * tok // clusters)
    slots = clusters * capacity
    labels = cluster_label[:, :, 0]
    earlier = jnp.arange(tok)[None, :] < jnp.arange(tok)[:, None]
    rank = jnp.sum(
        ((labels[:, :, None] == labels[:, None, :]) & earlier[None]).astype(jnp.int32), axis=2
    )
    aux = jnp.stack(
        [
            key_scale.T,
            value_scale.T,
            (labels * capacity).astype(jnp.bfloat16),
            rank.astype(jnp.bfloat16),
        ],
        axis=1,
    )
    aux = jnp.pad(aux, ((0, 0), (0, AUX - 4), (0, 0)))
    aux = aux.reshape(heads, AUX, tok // width, width).swapaxes(1, 2).reshape(heads, -1, width)
    packed = jnp.concatenate(
        [
            key_rows.swapaxes(0, 1),
            value_rows.swapaxes(0, 1),
            aux,
            queries.swapaxes(0, 1),
        ],
        axis=1,
    )
    vm = pl.BlockSpec(memory_space=pltpu.VMEM)
    dma = pltpu.SemaphoreType.DMA
    f32 = jnp.float32
    returned = pl.pallas_call(
        lambda *refs: exchange_kernel(chips, half, tok, slots, *refs),
        out_shape=jax.ShapeDtypeStruct((heads, tok, width), jnp.bfloat16),
        in_specs=[vm],
        out_specs=vm,
        scratch_shapes=[
            pltpu.VMEM((2 * chips,) + packed.shape[1:], jnp.bfloat16),
            pltpu.VMEM((chips, tok, width), jnp.bfloat16),
            pltpu.VMEM((2 * chips, slots, width), f32),
            pltpu.VMEM((2 * chips, slots, width), f32),
            pltpu.VMEM((2 * chips, slots, width), f32),
            pltpu.VMEM((chips, slots, width), f32),
            pltpu.VMEM((chips, slots, width), f32),
            pltpu.VMEM((slots // 8, 16 * chips, width), jnp.bfloat16),
            pltpu.VMEM((slots // 8, 16 * chips, width), jnp.bfloat16),
            pltpu.VMEM((slots // 8, 16, 16 * chips), f32),
            pltpu.VMEM((8 * chips, 16 * chips), f32),
        ]
        + [dma((chips,))] * 8,
        compiler_params=pltpu.CompilerParams(
            collective_id=0, has_side_effects=True, vmem_limit_bytes=62 * 1024 * 1024
        ),
        name="clustered",
    )(packed)
    return returned.swapaxes(0, 1)


UNROLL = 16
CHUNK = 4


def route(queries, key_rows, value_rows, key_scale, value_scale, cluster_label):
    tok, heads, width = queries.shape
    devices = lax.axis_size("outer") * lax.axis_size("inner")
    even = lax.axis_size("inner") % 2 == 0 and tok == 2 * width
    even = even and heads & (heads - 1) == 0 and heads % CHUNK == 0
    if devices == 2 * heads and even and 2 * tok == 4 * COARSE * FINE:
        return by_head(queries, key_rows, value_rows, key_scale, value_scale, cluster_label)
    return shards(queries, key_rows, value_rows, key_scale, value_scale, cluster_label)


def solution(mesh):
    placed = (
        P(("outer", "inner"), None, None),
        P(("outer", "inner"), None, None),
        P(("outer", "inner"), None, None),
        P(("outer", "inner"), None),
        P(("outer", "inner"), None),
        P(None, ("outer", "inner"), None),
    )
    return jax.shard_map(
        route,
        mesh=mesh,
        in_specs=placed,
        out_specs=P(("outer", "inner"), None, None),
        check_vma=False,
    )
```
